32 devices in a mesh: dp: 8 (over y, x, core), sp: 4 (over z).
Axes of the slice: x: 2, y: 2, z: 4, core: 2. Of those that a mesh axis runs over, the one named last changes fastest.
Arguments:
- queries: bfloat16 [4096, 8192], P(('dp', 'sp')), may hold values from -17.5 to 17.5
- key_rows: bfloat16 [4096, 1024], P(('dp', 'sp')), may hold values from -3.5 to 3.5
- value_rows: bfloat16 [4096, 1024], P(('dp', 'sp')), may hold values from -6 to 6
- grad_out: bfloat16 [4096, 8192], P(('dp', 'sp')), may hold values from -6 to 6
- doc_ids: int32 [4096], P(('dp', 'sp')), may hold values from 0 to 15, never falling along the last dimension, each value on 1 to 512 neighbouring positions
Outputs:
- attended: bfloat16 [4096, 8192], P(('dp', 'sp'))
- grad_queries: bfloat16 [4096, 8192], P(('dp', 'sp'))
- grad_keys: bfloat16 [4096, 1024], P(('dp', 'sp'))
- grad_values: bfloat16 [4096, 1024], P(('dp', 'sp'))
The draws below stay inside these ranges and needn't reach their ends.
Inputs may be any that keep to these rules, and one draw needn't show every extreme that they name: `doc_ids`: document numbers never fall along the tokens; every document has 1 to 512 tokens and one has exactly 512.
All inputs are finite; a program needn't handle non-finite values.
Results may differ from the reference program's by a relative error of at most 0.011.
Values may be sent and summed in bfloat16 or wider, within the bound.
A program may use at most 128 MiB of HBM per device.

```python
import math
import jax
import jax.numpy as jnp
import numpy as np
from jax import lax

H = 64
KV = 8
DH = 128
TOKENS = 4096
SPAN = 512


def shared_pair(key):
    seed_keys = jax.random.fold_in(key, 101)
    seed_queries = jax.random.fold_in(key, 202)
    key_group = jnp.clip(jax.random.normal(seed_keys, (TOKENS, KV, DH), jnp.float32), -3.4, 3.4)
    query_group = jnp.clip(jax.random.normal(seed_queries, (TOKENS, KV, H // KV, DH), jnp.float32), -3.4, 3.4)
    return (query_group.reshape(TOKENS, H * DH), key_group.reshape(TOKENS, KV * DH))


def draw_queries(key, part):
    return shared_pair(key)[0].astype(jnp.bfloat16)


def draw_key_rows(key, part):
    return shared_pair(key)[1].astype(jnp.bfloat16)


def block_levels(key, shape, cuts, least, largest):
    level = 1.0
    for position, blocks in cuts:
        steps = jax.random.uniform(jax.random.fold_in(jax.random.fold_in(key, 6), position), (blocks,), jnp.float32, least / len(cuts), largest / len(cuts))
        level = level * jnp.repeat(jnp.exp(steps), shape[position] // blocks).reshape((-1,) + (1,) * (len(shape) - 1 - position))
    return level


def split_up(count, total, most, slope):
    portions = [(1 << 20) // math.isqrt(standing ** slope) + 1 for standing in range(2, count + 1)]
    surplus, holding = total - most - (count - 1), [1] * (count - 1)
    while surplus > 0:
        free = [i for i in range(count - 1) if holding[i] < most]
        whole, budget = sum([portions[i] for i in free]), surplus
        for i in free:
            extra = min(most - holding[i], max(1, budget * portions[i] // whole), surplus)
            holding[i] = holding[i] + extra
            surplus = surplus - extra
    return np.array([most] + holding)


def ragged_sizes(rng, count, total, bound, skew):
    if count == 2:
        one = jax.random.randint(rng, (), max(1, total - bound), min(bound, total - 1) + 1)
        return jnp.stack([one, total - one])
    sizes = jnp.asarray(split_up(count, total, bound, skew), jnp.int32)
    pairs = (count - 1) // 2
    donor, taker = sizes[1:1 + 2 * pairs:2], sizes[2:2 + 2 * pairs:2]
    margin = jnp.minimum(donor - 1, bound - taker)
    passed = jax.random.randint(jax.random.fold_in(rng, 1), (pairs,), 0, 1 << 20) % (margin + 1)
    sizes = sizes.at[1:1 + 2 * pairs:2].set(donor - passed).at[2:2 + 2 * pairs:2].set(taker + passed)
    return sizes[jax.random.permutation(jax.random.fold_in(rng, 2), count)]


def gaussian(own_key, shape, scale, bound, pieces=(), kind=jnp.bfloat16):
    values = scale * jax.random.normal(own_key, shape, jnp.float32)
    if pieces:
        values = values * block_levels(own_key, shape, pieces, -0.22, 0.18)
    return jnp.clip(values, -bound, bound).astype(kind)


def setup_inputs(seed: int = 0) -> dict:
    key_of = jax.random.split(jax.random.key(seed), 6)
    queries = draw_queries(jax.random.fold_in(key_of[5], 71), 0)
    key_rows = draw_key_rows(jax.random.fold_in(key_of[5], 71), 0)
    value_rows = gaussian(key_of[2], (TOKENS, KV * DH), 1.0, 6.0, ((0, 32),))
    grad_out = gaussian(key_of[3], (TOKENS, H * DH), 1.0, 6.0, ((0, 32),))
    doc_ids = jnp.searchsorted(jnp.cumsum(ragged_sizes(key_of[4], 2 * TOKENS // SPAN, TOKENS, SPAN, 1)), jnp.arange(TOKENS), side="right").astype(jnp.int32)
    return {"queries": queries, "key_rows": key_rows, "value_rows": value_rows, "grad_out": grad_out, "doc_ids": doc_ids}


NEGATIVE = -1e30


def band_mask(query_docs, query_pos, key_docs, key_pos):
    same = query_docs[:, None] == key_docs[None, :]
    return same & (key_pos[None, :] <= query_pos[:, None]) & (key_pos[None, :] >= 0)


def group_all(items, mask):
    query_group, key_group, value_group, grad_group = items
    query_float = query_group.astype(jnp.float32)
    key_float = key_group.astype(jnp.float32)
    value_float = value_group.astype(jnp.float32)
    grad_float = grad_group.astype(jnp.float32)
    scores = jnp.einsum("qhd,wd->hqw", query_float, key_float) * (DH ** -0.5)
    scores = jnp.where(mask[None], scores, NEGATIVE)
    expo = jnp.exp(scores - jnp.max(scores, axis=-1, keepdims=True))
    probs = expo / jnp.sum(expo, axis=-1, keepdims=True)
    weights = probs.astype(jnp.bfloat16)
    output = jnp.einsum("hqw,wd->qhd", weights.astype(jnp.float32), value_float).astype(jnp.bfloat16)
    dprobs = jnp.einsum("qhd,wd->hqw", grad_float, value_float)
    delta = jnp.sum(grad_float * output.astype(jnp.float32), axis=-1).T
    dscores = (probs * (dprobs - delta[:, :, None]) * (DH ** -0.5)).astype(jnp.bfloat16)
    dscore_float = dscores.astype(jnp.float32)
    grad_query = jnp.einsum("hqw,wd->qhd", dscore_float, key_float).astype(jnp.bfloat16)
    grad_key = jnp.einsum("hqw,qhd->wd", dscore_float, query_float)
    grad_value = jnp.einsum("hqw,qhd->wd", weights.astype(jnp.float32), grad_float)
    return output, grad_query, grad_key, grad_value


def reference(queries, key_rows, value_rows, grad_out, doc_ids):
    block_rows = min(512, SPAN)
    width = SPAN + block_rows
    per_group = H // KV
    pad_keys = jnp.concatenate([jnp.zeros((SPAN, KV * DH), jnp.bfloat16), key_rows], axis=0)
    pad_values = jnp.concatenate([jnp.zeros((SPAN, KV * DH), jnp.bfloat16), value_rows], axis=0)
    pad_docs = jnp.concatenate([jnp.full((SPAN,), -1, jnp.int32), doc_ids], axis=0)

    def advance(carry, step):
        key_acc, value_acc = carry
        start = (step * block_rows).astype(jnp.int32)
        query_block = lax.dynamic_slice_in_dim(queries, start, block_rows, 0).reshape(block_rows, KV, per_group, DH).transpose(1, 0, 2, 3)
        grad_block = lax.dynamic_slice_in_dim(grad_out, start, block_rows, 0).reshape(block_rows, KV, per_group, DH).transpose(1, 0, 2, 3)
        key_window = lax.dynamic_slice_in_dim(pad_keys, start, width, 0).reshape(width, KV, DH).transpose(1, 0, 2)
        value_window = lax.dynamic_slice_in_dim(pad_values, start, width, 0).reshape(width, KV, DH).transpose(1, 0, 2)
        query_pos = start + jnp.arange(block_rows, dtype=jnp.int32)
        key_pos = start - SPAN + jnp.arange(width, dtype=jnp.int32)
        mask = band_mask(lax.dynamic_slice_in_dim(doc_ids, start, block_rows, 0), query_pos,
                         lax.dynamic_slice_in_dim(pad_docs, start, width, 0), key_pos)
        outputs, grad_qs, grad_ks, grad_vs = lax.map(lambda items: group_all(items, mask),
                                                     (query_block, key_window, value_window, grad_block))
        key_part = grad_ks.transpose(1, 0, 2).reshape(width, KV * DH)
        value_part = grad_vs.transpose(1, 0, 2).reshape(width, KV * DH)
        key_acc = lax.dynamic_update_slice_in_dim(key_acc, lax.dynamic_slice_in_dim(key_acc, start, width, 0) + key_part, start, 0)
        value_acc = lax.dynamic_update_slice_in_dim(value_acc, lax.dynamic_slice_in_dim(value_acc, start, width, 0) + value_part, start, 0)
        return (key_acc, value_acc), (outputs.transpose(1, 0, 2, 3).reshape(block_rows, H * DH),
                                      grad_qs.transpose(1, 0, 2, 3).reshape(block_rows, H * DH))

    zeros = jnp.zeros((SPAN + TOKENS, KV * DH), jnp.float32)
    (key_acc, value_acc), (attended, grad_queries) = lax.scan(advance, (zeros, zeros), jnp.arange(TOKENS // block_rows, dtype=jnp.int32))
    attended = attended.reshape(TOKENS, H * DH)
    grad_queries = grad_queries.reshape(TOKENS, H * DH)
    return attended, grad_queries, key_acc[SPAN:].astype(jnp.bfloat16), value_acc[SPAN:].astype(jnp.bfloat16)
```

```python
import functools
import math

import jax
import jax.numpy as jnp
from jax import lax
from jax.experimental import pallas as pl
from jax.experimental.pallas import tpu as pltpu
from jax.sharding import PartitionSpec as P

DH = 128
NEGATIVE = -1e30
MESH = pl.DeviceIdType.MESH
PAIR = 2


def kernel(
    ndp, nsp, groups, heads,
    q_hbm, k_hbm, v_hbm, g_hbm, ids_hbm,
    att_hbm, gq_hbm, gk_hbm, gv_hbm,
    q_buf, g_buf, att_buf, gq_buf, kv_buf, ids_buf, bias, pt_buf, ds_buf,
    part_own, part_send, part_recv, gk_buf, gv_buf,
    load_sem, out_sem, kv_load, kv_send, kv_recv, ids_send, ids_recv, ids_load,
    pg_send, pg_recv, fin_sem,
):
    me = lax.axis_index("dp") * nsp + lax.axis_index("sp")
    total = ndp * nsp
    blocks = nsp + 1
    rows = q_hbm.shape[0]
    scale = DH ** (-0.5)

    def device(index):
        return (index // nsp, lax.rem(index, nsp))

    def head_cols(g):
        return pl.ds(pl.multiple_of(g * (heads * DH), heads * DH), heads * DH)

    def key_cols(g):
        return pl.ds(pl.multiple_of(g * DH, DH), DH)

    def load_k(g):
        return pltpu.make_async_copy(k_hbm.at[:, key_cols(g)], kv_buf.at[g, nsp, 0], kv_load.at[g, 0])

    def load_v(g):
        return pltpu.make_async_copy(v_hbm.at[:, key_cols(g)], kv_buf.at[g, nsp, 1], kv_load.at[g, 1])

    def load_q(g):
        return pltpu.make_async_copy(q_hbm.at[:, head_cols(g)], q_buf.at[g], load_sem.at[g, 0])

    def load_g(g):
        return pltpu.make_async_copy(g_hbm.at[:, head_cols(g)], g_buf.at[g], load_sem.at[g, 1])

    def store_att(g):
        return pltpu.make_async_copy(att_buf.at[g], att_hbm.at[:, head_cols(g)], out_sem.at[g, 0])

    def store_gq(g):
        return pltpu.make_async_copy(gq_buf.at[g], gq_hbm.at[:, head_cols(g)], out_sem.at[g, 1])

    def send_kv(g, dist):
        return pltpu.make_async_remote_copy(
            src_ref=kv_buf.at[g, nsp], dst_ref=kv_buf.at[g, nsp - dist],
            send_sem=kv_send.at[g, dist - 1], recv_sem=kv_recv.at[g, dist - 1],
            device_id=device(me + dist), device_id_type=MESH)

    def send_ids(dist):
        return pltpu.make_async_remote_copy(
            src_ref=ids_buf.at[nsp], dst_ref=ids_buf.at[nsp - dist],
            send_sem=ids_send.at[dist - 1], recv_sem=ids_recv.at[dist - 1],
            device_id=device(me + dist), device_id_type=MESH)

    def send_part(g, dist):
        return pltpu.make_async_remote_copy(
            src_ref=part_send.at[g, dist - 1], dst_ref=part_recv.at[g, dist - 1],
            send_sem=pg_send.at[g, dist - 1], recv_sem=pg_recv.at[g, dist - 1],
            device_id=device(me - dist), device_id_type=MESH)

    ids_copy = pltpu.make_async_copy(ids_hbm, ids_buf.at[nsp], ids_load)
    ids_copy.start()
    for g in range(groups):
        load_k(g).start()
        load_v(g).start()
    for g in range(groups):
        load_q(g).start()
        load_g(g).start()

    barrier = pltpu.get_barrier_semaphore()
    for dist in range(1, nsp + 1):
        @pl.when(me + dist < total)
        def _():
            pl.semaphore_signal(barrier, inc=1, device_id=device(me + dist), device_id_type=MESH)

        @pl.when(me - dist >= 0)
        def _():
            pl.semaphore_signal(barrier, inc=1, device_id=device(me - dist), device_id_type=MESH)

    peers = jnp.minimum(nsp, total - 1 - me) + jnp.minimum(nsp, me)
    pl.semaphore_wait(barrier, peers)

    ids_copy.wait()
    for dist in range(1, nsp + 1):
        @pl.when(me + dist < total)
        def _():
            send_ids(dist).start()

    def start_kv(g, carry):
        load_k(g).wait()
        load_v(g).wait()
        for dist in range(1, nsp + 1):
            @pl.when(me + dist < total)
            def _():
                send_kv(g, dist).start()
        return carry

    lax.fori_loop(0, groups, start_kv, 0)

    for dist in range(1, nsp + 1):
        @pl.when(me - dist < 0)
        def _():
            ids_buf[nsp - dist] = jnp.full((8, rows), -1.0, jnp.float32)

            def clear(g, carry):
                kv_buf[g, nsp - dist] = jnp.zeros((2, rows, DH), jnp.bfloat16)
                return carry

            lax.fori_loop(0, groups, clear, 0)

        @pl.when(me - dist >= 0)
        def _():
            send_ids(dist).wait_recv()

    own = jnp.broadcast_to(ids_buf[nsp][0:1], (rows, rows))
    for slot in range(blocks):
        other = jnp.broadcast_to(ids_buf[slot][0:1], (rows, rows)).T
        allowed = other == own
        if slot == nsp:
            key_pos = lax.broadcasted_iota(jnp.int32, (rows, rows), 0)
            query_pos = lax.broadcasted_iota(jnp.int32, (rows, rows), 1)
            allowed = allowed & (key_pos <= query_pos)
        bias[slot * rows:(slot + 1) * rows, :] = jnp.where(allowed, 0.0, NEGATIVE)

    width = blocks * rows
    factor = scale * math.log2(math.e)

    def group_step(g, carry):
        load_q(g).wait()
        load_g(g).wait()
        for dist in range(1, nsp + 1):
            @pl.when(me - dist >= 0)
            def _():
                send_kv(g, dist).wait_recv()

        keys = kv_buf[g, :, 0].reshape(width, DH)
        values = kv_buf[g, :, 1].reshape(width, DH)
        keys_t = keys.T
        values_t = values.T
        for pair in range(heads // PAIR):
            first = pair * PAIR

            def stacked(buf):
                return jnp.concatenate(
                    [buf[g, :, (first + i) * DH:(first + i + 1) * DH] for i in range(PAIR)], axis=0)

            queries = stacked(q_buf)
            grads = stacked(g_buf)
            wide_bias = jnp.concatenate([bias[...]] * PAIR, axis=1)
            nt = (((1,), (1,)), ((), ()))
            scores = lax.dot_general(keys, queries, nt, preferred_element_type=jnp.float32) + wide_bias
            top = jnp.max(scores, axis=0, keepdims=True)
            expo = jnp.exp2((scores - top) * factor)
            probs = expo * (1.0 / jnp.sum(expo, axis=0, keepdims=True))
            weights = probs.astype(jnp.bfloat16)
            pt_buf[:, first * rows:(first + PAIR) * rows] = weights
            out_t = jnp.dot(values_t, weights, preferred_element_type=jnp.float32)
            dprobs = lax.dot_general(values, grads, nt, preferred_element_type=jnp.float32)
            delta = jnp.sum(probs * dprobs, axis=0, keepdims=True)
            dscores = (probs * (dprobs - delta)).astype(jnp.bfloat16)
            ds_buf[:, first * rows:(first + PAIR) * rows] = dscores
            grad_t = jnp.dot(keys_t, dscores, preferred_element_type=jnp.float32) * scale
            for i in range(PAIR):
                cols = slice((first + i) * DH, (first + i + 1) * DH)
                att_buf[g, :, cols] = out_t[:, i * rows:(i + 1) * rows].T.astype(jnp.bfloat16)
                gq_buf[g, :, cols] = grad_t[:, i * rows:(i + 1) * rows].T.astype(jnp.bfloat16)

        store_att(g).start()
        store_gq(g).start()
        all_q = jnp.concatenate([q_buf[g, :, h * DH:(h + 1) * DH] for h in range(heads)], axis=0)
        all_g = jnp.concatenate([g_buf[g, :, h * DH:(h + 1) * DH] for h in range(heads)], axis=0)
        for slot in range(blocks):
            part = slice(slot * rows, (slot + 1) * rows)
            grad_k = jnp.dot(ds_buf[part, :], all_q, preferred_element_type=jnp.float32) * scale
            grad_v = jnp.dot(pt_buf[part, :], all_g, preferred_element_type=jnp.float32)
            if slot == nsp:
                part_own[g, 0] = grad_k
                part_own[g, 1] = grad_v
            else:
                part_send[g, nsp - slot - 1, 0] = grad_k.astype(jnp.bfloat16)
                part_send[g, nsp - slot - 1, 1] = grad_v.astype(jnp.bfloat16)
        for dist in range(1, nsp + 1):
            @pl.when(me - dist >= 0)
            def _():
                send_part(g, dist).start()
        return carry

    lax.fori_loop(0, groups, group_step, 0)

    for dist in range(1, nsp + 1):
        @pl.when(me + dist >= total)
        def _():
            def clear(g, carry):
                part_recv[g, dist - 1] = jnp.zeros((2, rows, DH), jnp.bfloat16)
                return carry

            lax.fori_loop(0, groups, clear, 0)

    def finish(g, carry):
        for dist in range(1, nsp + 1):
            @pl.when(me + dist < total)
            def _():
                send_part(g, dist).wait_recv()

        acc = part_own[g]
        for dist in range(1, nsp + 1):
            acc = acc + part_recv[g, dist - 1].astype(jnp.float32)
        acc = acc.astype(jnp.bfloat16)
        gk_buf[g] = acc[0]
        gv_buf[g] = acc[1]
        pltpu.make_async_copy(gk_buf.at[g], gk_hbm.at[:, key_cols(g)], fin_sem.at[g, 0]).start()
        pltpu.make_async_copy(gv_buf.at[g], gv_hbm.at[:, key_cols(g)], fin_sem.at[g, 1]).start()
        return carry

    lax.fori_loop(0, groups, finish, 0)

    def drain(g, carry):
        store_att(g).wait()
        store_gq(g).wait()
        pltpu.make_async_copy(gk_buf.at[g], gk_hbm.at[:, key_cols(g)], fin_sem.at[g, 0]).wait()
        pltpu.make_async_copy(gv_buf.at[g], gv_hbm.at[:, key_cols(g)], fin_sem.at[g, 1]).wait()
        for dist in range(1, nsp + 1):
            @pl.when(me + dist < total)
            def _():
                send_kv(g, dist).wait_send()

            @pl.when(me - dist >= 0)
            def _():
                send_part(g, dist).wait_send()
        return carry

    lax.fori_loop(0, groups, drain, 0)
    for dist in range(1, nsp + 1):
        @pl.when(me + dist < total)
        def _():
            send_ids(dist).wait_send()


def shards(queries, key_rows, value_rows, grad_out, doc_ids):
    ndp, nsp = lax.axis_size("dp"), lax.axis_size("sp")
    rows = queries.shape[0]
    groups = key_rows.shape[1] // DH
    heads = queries.shape[1] // key_rows.shape[1]
    blocks = nsp + 1
    ids = jnp.broadcast_to(doc_ids.astype(jnp.float32)[None, :], (8, rows))
    bf16, f32 = jnp.bfloat16, jnp.float32
    hbm = pl.BlockSpec(memory_space=pl.ANY)
    dma = pltpu.SemaphoreType.DMA
    return pl.pallas_call(
        functools.partial(kernel, ndp, nsp, groups, heads),
        out_shape=(
            jax.ShapeDtypeStruct(queries.shape, bf16),
            jax.ShapeDtypeStruct(queries.shape, bf16),
            jax.ShapeDtypeStruct(key_rows.shape, bf16),
            jax.ShapeDtypeStruct(key_rows.shape, bf16),
        ),
        in_specs=[hbm] * 5,
        out_specs=(hbm,) * 4,
        scratch_shapes=[
            pltpu.VMEM((groups, rows, heads * DH), bf16),
            pltpu.VMEM((groups, rows, heads * DH), bf16),
            pltpu.VMEM((groups, rows, heads * DH), bf16),
            pltpu.VMEM((groups, rows, heads * DH), bf16),
            pltpu.VMEM((groups, blocks, 2, rows, DH), bf16),
            pltpu.VMEM((blocks, 8, rows), f32),
            pltpu.VMEM((blocks * rows, rows), f32),
            pltpu.VMEM((blocks * rows, heads * rows), bf16),
            pltpu.VMEM((blocks * rows, heads * rows), bf16),
            pltpu.VMEM((groups, 2, rows, DH), f32),
            pltpu.VMEM((groups, nsp, 2, rows, DH), bf16),
            pltpu.VMEM((groups, nsp, 2, rows, DH), bf16),
            pltpu.VMEM((groups, rows, DH), bf16),
            pltpu.VMEM((groups, rows, DH), bf16),
            dma((groups, 2)),
            dma((groups, 2)),
            dma((groups, 2)),
            dma((groups, nsp)),
            dma((groups, nsp)),
            dma((nsp,)),
            dma((nsp,)),
            dma,
            dma((groups, nsp)),
            dma((groups, nsp)),
            dma((groups, 2)),
        ],
        compiler_params=pltpu.CompilerParams(
            collective_id=0, has_side_effects=True, vmem_limit_bytes=60 * 1024 * 1024),
        name="attention",
    )(queries, key_rows, value_rows, grad_out, ids)


def solution(mesh):
    rows = P(("dp", "sp"), None)
    return jax.shard_map(
        shards,
        mesh=mesh,
        in_specs=(rows, rows, rows, rows, P(("dp", "sp"))),
        out_specs=(rows, rows, rows, rows),
        check_vma=False,
    )
```

```python
import functools
import math

import jax
import jax.numpy as jnp
from jax import lax
from jax.experimental import pallas as pl
from jax.experimental.pallas import tpu as pltpu
from jax.sharding import PartitionSpec as P

DH = 128
NEGATIVE = -1e30
MESH = pl.DeviceIdType.MESH
PAIR = 2


def kernel(
    ndp, nsp, groups, heads,
    q_hbm, k_hbm, v_hbm, g_hbm, ids_hbm,
    att_hbm, gq_hbm, gk_hbm, gv_hbm,
    q_buf, g_buf, att_buf, gq_buf, kv_buf, ids_buf, bias, pt_buf, ds_buf,
    part_own, part_send, part_recv, gk_buf, gv_buf,
    load_sem, out_sem, kv_load, kv_send, kv_recv, ids_send, ids_recv, ids_load,
    pg_send, pg_recv, fin_sem,
):
    row, col = lax.axis_index("dp"), lax.axis_index("sp")
    blocks = nsp + 1
    rows = q_hbm.shape[0]
    scale = DH ** (-0.5)

    def head_cols(g):
        return pl.ds(pl.multiple_of(g * (heads * DH), heads * DH), heads * DH)

    def key_cols(g):
        return pl.ds(pl.multiple_of(g * DH, DH), DH)

    def load_k(g):
        return pltpu.make_async_copy(k_hbm.at[:, key_cols(g)], kv_buf.at[g, nsp, 0], kv_load.at[g, 0])

    def load_v(g):
        return pltpu.make_async_copy(v_hbm.at[:, key_cols(g)], kv_buf.at[g, nsp, 1], kv_load.at[g, 1])

    def load_q(g):
        return pltpu.make_async_copy(q_hbm.at[:, head_cols(g)], q_buf.at[g], load_sem.at[g, 0])

    def load_g(g):
        return pltpu.make_async_copy(g_hbm.at[:, head_cols(g)], g_buf.at[g], load_sem.at[g, 1])

    def store_att(g):
        return pltpu.make_async_copy(att_buf.at[g], att_hbm.at[:, head_cols(g)], out_sem.at[g, 0])

    def store_gq(g):
        return pltpu.make_async_copy(gq_buf.at[g], gq_hbm.at[:, head_cols(g)], out_sem.at[g, 1])

    def remote(src, dst, send_sem, recv_sem, target):
        return pltpu.make_async_remote_copy(
            src_ref=src, dst_ref=dst, send_sem=send_sem, recv_sem=recv_sem,
            device_id=target, device_id_type=MESH)

    up, down, later, earlier = (row, col + 1), (row, col - 1), (row + 1, col), (row - 1, col)
    has_up, has_down, has_later, has_earlier = col + 1 < nsp, col >= 1, row + 1 < ndp, row >= 1

    def kv_up(g, dist):
        return remote(kv_buf.at[g, nsp - dist], kv_buf.at[g, nsp - dist - 1],
                      kv_send.at[g, dist], kv_recv.at[g, dist], up)

    def kv_down(g, dist):
        return remote(kv_buf.at[g, nsp - dist], kv_buf.at[g, nsp - dist + 1],
                      kv_send.at[g, dist], kv_recv.at[g, dist - 2], down)

    def kv_later(g):
        return remote(kv_buf.at[g, nsp], kv_buf.at[g, 0],
                      kv_send.at[g, nsp + 1], kv_recv.at[g, nsp - 1], later)

    def arrived(g, dist):
        return remote(kv_buf.at[g, nsp], kv_buf.at[g, nsp - dist],
                      kv_send.at[g, 0], kv_recv.at[g, dist - 1], up)

    def part_down(g, dist):
        return remote(part_send.at[g, dist - 1], part_recv.at[g, dist - 1],
                      pg_send.at[g, dist - 1], pg_recv.at[g, dist - 1], down)

    def part_up(g, dist):
        return remote(part_send.at[g, dist - 1], part_recv.at[g, dist + 1],
                      pg_send.at[g, dist - 1], pg_recv.at[g, dist + 1], up)

    def part_earlier(g):
        return remote(part_send.at[g, nsp - 1], part_recv.at[g, nsp + 1],
                      pg_send.at[g, nsp - 1], pg_recv.at[g, nsp + 1], earlier)

    def part_sent(g, dist):
        return remote(part_send.at[g, dist - 1], part_recv.at[g, 0],
                      pg_send.at[g, dist - 1], pg_recv.at[g, 0], up)

    def part_arrived(g, slot):
        return remote(part_send.at[g, 0], part_recv.at[g, slot],
                      pg_send.at[g, 0], pg_recv.at[g, slot], up)

    def ids_to(dist, target):
        return remote(ids_buf.at[nsp], ids_buf.at[nsp - dist],
                      ids_send.at[dist - 1], ids_recv.at[dist - 1], target)

    def ids_target(dist):
        index = row * nsp + col + dist
        return (index // nsp, lax.rem(index, nsp))

    def ids_source(dist):
        index = row * nsp + col - dist
        return (index // nsp, lax.rem(index, nsp))

    def sends_ids(dist):
        return row * nsp + col + dist < ndp * nsp

    def gets_ids(dist):
        return row * nsp + col - dist >= 0

    def own_out(g):
        load_k(g).wait()
        load_v(g).wait()

        @pl.when(has_up)
        def _():
            kv_up(g, 0).start()

        @pl.when(has_later)
        def _():
            kv_later(g).start()

    def gather(g, stage):
        @pl.when(col >= stage)
        def _():
            arrived(g, stage).wait_recv()

            if stage < nsp:
                @pl.when(has_up)
                def _():
                    kv_up(g, stage).start()

        dist = nsp + 1 - stage

        @pl.when(has_earlier & (col < dist))
        def _():
            arrived(g, dist).wait_recv()

            if dist >= 2:
                @pl.when(has_down)
                def _():
                    kv_down(g, dist).start()

    def add_part(g, dist):
        part_arrived(g, dist).wait_recv()
        mine = part_send[g, dist - 1].astype(jnp.float32)
        theirs = part_recv[g, dist].astype(jnp.float32)
        part_send[g, dist - 1] = (mine + theirs).astype(jnp.bfloat16)

    def scatter_down(g):
        for dist in range(1, nsp):
            @pl.when(col >= dist)
            def _():
                @pl.when(has_up)
                def _():
                    add_part(g, dist)

                part_down(g, dist).start()

    def scatter_up(g):
        for dist in range(nsp, 0, -1):
            @pl.when(has_earlier & (col < dist))
            def _():
                @pl.when(has_down)
                def _():
                    add_part(g, dist)

                if dist == nsp:
                    part_earlier(g).start()
                else:
                    part_up(g, dist).start()

    ids_copy = pltpu.make_async_copy(ids_hbm, ids_buf.at[nsp], ids_load)
    ids_copy.start()
    for g in range(groups):
        load_k(g).start()
        load_v(g).start()
    for g in range(groups):
        load_q(g).start()
        load_g(g).start()

    barrier = pltpu.get_barrier_semaphore()
    for dist in range(1, nsp + 1):
        @pl.when(sends_ids(dist))
        def _():
            pl.semaphore_signal(barrier, inc=1, device_id=ids_target(dist), device_id_type=MESH)

        @pl.when(gets_ids(dist))
        def _():
            pl.semaphore_signal(barrier, inc=1, device_id=ids_source(dist), device_id_type=MESH)

    place = row * nsp + col
    peers = jnp.minimum(nsp, ndp * nsp - 1 - place) + jnp.minimum(nsp, place)
    pl.semaphore_wait(barrier, peers)

    ids_copy.wait()
    for dist in range(1, nsp + 1):
        @pl.when(sends_ids(dist))
        def _():
            ids_to(dist, ids_target(dist)).start()

    for dist in range(1, nsp + 1):
        @pl.when(jnp.logical_not(gets_ids(dist)))
        def _():
            ids_buf[nsp - dist] = jnp.full((8, rows), -1.0, jnp.float32)

            def clear(g, carry):
                kv_buf[g, nsp - dist] = jnp.zeros((2, rows, DH), jnp.bfloat16)
                return carry

            lax.fori_loop(0, groups, clear, 0)

    own_out(0)
    for dist in range(1, nsp + 1):
        @pl.when(gets_ids(dist))
        def _():
            ids_to(dist, up).wait_recv()

    own = jnp.broadcast_to(ids_buf[nsp][0:1], (rows, rows))
    for slot in range(blocks):
        other = jnp.broadcast_to(ids_buf[slot][0:1], (rows, rows)).T
        allowed = other == own
        if slot == nsp:
            key_pos = lax.broadcasted_iota(jnp.int32, (rows, rows), 0)
            query_pos = lax.broadcasted_iota(jnp.int32, (rows, rows), 1)
            allowed = allowed & (key_pos <= query_pos)
        bias[slot * rows:(slot + 1) * rows, :] = jnp.where(allowed, 0.0, NEGATIVE)

    width = blocks * rows
    factor = scale * math.log2(math.e)

    def compute(g):
        load_q(g).wait()
        load_g(g).wait()
        keys = kv_buf[g, :, 0].reshape(width, DH)
        values = kv_buf[g, :, 1].reshape(width, DH)
        keys_t = keys.T
        values_t = values.T
        for pair in range(heads // PAIR):
            first = pair * PAIR

            def stacked(buf):
                return jnp.concatenate(
                    [buf[g, :, (first + i) * DH:(first + i + 1) * DH] for i in range(PAIR)], axis=0)

            queries = stacked(q_buf)
            grads = stacked(g_buf)
            wide_bias = jnp.concatenate([bias[...]] * PAIR, axis=1)
            nt = (((1,), (1,)), ((), ()))
            scores = lax.dot_general(keys, queries, nt, preferred_element_type=jnp.float32) + wide_bias
            top = jnp.max(scores, axis=0, keepdims=True)
            expo = jnp.exp2((scores - top) * factor)
            probs = expo * (1.0 / jnp.sum(expo, axis=0, keepdims=True))
            weights = probs.astype(jnp.bfloat16)
            pt_buf[:, first * rows:(first + PAIR) * rows] = weights
            out_t = jnp.dot(values_t, weights, preferred_element_type=jnp.float32)
            dprobs = lax.dot_general(values, grads, nt, preferred_element_type=jnp.float32)
            delta = jnp.sum(probs * dprobs, axis=0, keepdims=True)
            dscores = (probs * (dprobs - delta)).astype(jnp.bfloat16)
            ds_buf[:, first * rows:(first + PAIR) * rows] = dscores
            grad_t = jnp.dot(keys_t, dscores, preferred_element_type=jnp.float32) * scale
            for i in range(PAIR):
                cols = slice((first + i) * DH, (first + i + 1) * DH)
                att_buf[g, :, cols] = out_t[:, i * rows:(i + 1) * rows].T.astype(jnp.bfloat16)
                gq_buf[g, :, cols] = grad_t[:, i * rows:(i + 1) * rows].T.astype(jnp.bfloat16)

        store_att(g).start()
        store_gq(g).start()
        all_q = jnp.concatenate([q_buf[g, :, h * DH:(h + 1) * DH] for h in range(heads)], axis=0)
        all_g = jnp.concatenate([g_buf[g, :, h * DH:(h + 1) * DH] for h in range(heads)], axis=0)
        for slot in range(blocks):
            part = slice(slot * rows, (slot + 1) * rows)
            grad_k = jnp.dot(ds_buf[part, :], all_q, preferred_element_type=jnp.float32) * scale
            grad_v = jnp.dot(pt_buf[part, :], all_g, preferred_element_type=jnp.float32)
            if slot == nsp:
                part_own[g, 0] = grad_k
                part_own[g, 1] = grad_v
            else:
                part_send[g, nsp - slot - 1, 0] = grad_k.astype(jnp.bfloat16)
                part_send[g, nsp - slot - 1, 1] = grad_v.astype(jnp.bfloat16)

    def step(g, carry):
        @pl.when((g + nsp >= 1) & (g + nsp < groups))
        def _():
            own_out(g + nsp)

        for stage in range(1, nsp + 1):
            ahead = g + nsp - stage

            @pl.when((ahead >= 0) & (ahead < groups))
            def _():
                gather(ahead, stage)

        @pl.when((g >= 0) & (g < groups))
        def _():
            compute(g)

        lower = g - (nsp - 1 - col)

        @pl.when((lower >= 0) & (lower < groups))
        def _():
            scatter_down(lower)

        upper = g - col

        @pl.when((upper >= 0) & (upper < groups))
        def _():
            scatter_up(upper)

        return carry

    lax.fori_loop(1 - nsp, groups + nsp - 1, step, 0)

    for have, slot in ((has_up, 0), (has_later, nsp + 1)):
        @pl.when(jnp.logical_not(have))
        def _():
            def clear(g, carry):
                part_recv[g, slot] = jnp.zeros((2, rows, DH), jnp.bfloat16)
                return carry

            lax.fori_loop(0, groups, clear, 0)

    def finish(g, carry):
        for have, slot in ((has_up, 0), (has_later, nsp + 1)):
            @pl.when(have)
            def _():
                part_arrived(g, slot).wait_recv()

        acc = part_own[g]
        for slot in (0, nsp + 1):
            acc = acc + part_recv[g, slot].astype(jnp.float32)
        acc = acc.astype(jnp.bfloat16)
        gk_buf[g] = acc[0]
        gv_buf[g] = acc[1]
        pltpu.make_async_copy(gk_buf.at[g], gk_hbm.at[:, key_cols(g)], fin_sem.at[g, 0]).start()
        pltpu.make_async_copy(gv_buf.at[g], gv_hbm.at[:, key_cols(g)], fin_sem.at[g, 1]).start()
        return carry

    lax.fori_loop(0, groups, finish, 0)

    def drain(g, carry):
        store_att(g).wait()
        store_gq(g).wait()
        pltpu.make_async_copy(gk_buf.at[g], gk_hbm.at[:, key_cols(g)], fin_sem.at[g, 0]).wait()
        pltpu.make_async_copy(gv_buf.at[g], gv_hbm.at[:, key_cols(g)], fin_sem.at[g, 1]).wait()
        @pl.when(has_up)
        def _():
            kv_up(g, 0).wait_send()

        @pl.when(has_later)
        def _():
            kv_later(g).wait_send()

        for dist in range(1, nsp + 1):
            @pl.when((col >= dist) & has_up)
            def _():
                kv_up(g, min(dist, nsp - 1)).wait_send()

            @pl.when(has_earlier & (col < dist) & has_down)
            def _():
                kv_down(g, max(dist, 2)).wait_send()

            @pl.when((col >= dist) | has_earlier)
            def _():
                part_sent(g, dist).wait_send()

        return carry

    lax.fori_loop(0, groups, drain, 0)
    for dist in range(1, nsp + 1):
        @pl.when(sends_ids(dist))
        def _():
            ids_to(dist, ids_target(dist)).wait_send()


def shards(queries, key_rows, value_rows, grad_out, doc_ids):
    ndp, nsp = lax.axis_size("dp"), lax.axis_size("sp")
    rows = queries.shape[0]
    groups = key_rows.shape[1] // DH
    heads = queries.shape[1] // key_rows.shape[1]
    blocks = nsp + 1
    ids = jnp.broadcast_to(doc_ids.astype(jnp.float32)[None, :], (8, rows))
    bf16, f32 = jnp.bfloat16, jnp.float32
    hbm = pl.BlockSpec(memory_space=pl.ANY)
    dma = pltpu.SemaphoreType.DMA
    return pl.pallas_call(
        functools.partial(kernel, ndp, nsp, groups, heads),
        out_shape=(
            jax.ShapeDtypeStruct(queries.shape, bf16),
            jax.ShapeDtypeStruct(queries.shape, bf16),
            jax.ShapeDtypeStruct(key_rows.shape, bf16),
            jax.ShapeDtypeStruct(key_rows.shape, bf16),
        ),
        in_specs=[hbm] * 5,
        out_specs=(hbm,) * 4,
        scratch_shapes=[
            pltpu.VMEM((groups, rows, heads * DH), bf16),
            pltpu.VMEM((groups, rows, heads * DH), bf16),
            pltpu.VMEM((groups, rows, heads * DH), bf16),
            pltpu.VMEM((groups, rows, heads * DH), bf16),
            pltpu.VMEM((groups, blocks, 2, rows, DH), bf16),
            pltpu.VMEM((blocks, 8, rows), f32),
            pltpu.VMEM((blocks * rows, rows), f32),
            pltpu.VMEM((blocks * rows, heads * rows), bf16),
            pltpu.VMEM((blocks * rows, heads * rows), bf16),
            pltpu.VMEM((groups, 2, rows, DH), f32),
            pltpu.VMEM((groups, nsp, 2, rows, DH), bf16),
            pltpu.VMEM((groups, nsp + 2, 2, rows, DH), bf16),
            pltpu.VMEM((groups, rows, DH), bf16),
            pltpu.VMEM((groups, rows, DH), bf16),
            dma((groups, 2)),
            dma((groups, 2)),
            dma((groups, 2)),
            dma((groups, nsp + 2)),
            dma((groups, nsp)),
            dma((nsp,)),
            dma((nsp,)),
            dma,
            dma((groups, nsp)),
            dma((groups, nsp + 2)),
            dma((groups, 2)),
        ],
        compiler_params=pltpu.CompilerParams(
            collective_id=0, has_side_effects=True, vmem_limit_bytes=60 * 1024 * 1024),
        name="attention",
    )(queries, key_rows, value_rows, grad_out, ids)


def solution(mesh):
    rows = P(("dp", "sp"), None)
    return jax.shard_map(
        shards,
        mesh=mesh,
        in_specs=(rows, rows, rows, rows, P(("dp", "sp"))),
        out_specs=(rows, rows, rows, rows),
        check_vma=False,
    )
```
